512 devices in a mesh: wide: 32 (over z, x_hi), narrow: 16 (over y, x_lo, core).
Axes of the slice: x: 4 (x_hi: 2, x_lo: 2; x = x_hi * 2 + x_lo), y: 4, z: 16, core: 2. Of those that a mesh axis runs over, the one named last changes fastest.
Arguments:
- moments: float32 [16384, 2048], P('wide', 'narrow'), as said below
- eigen_basis: float32 [16384, 2048], P('wide', 'narrow'), may hold values from -0.125 to 0.125
- slot_order: int32 [8], replicated, may hold values 0 or 1
Outputs:
- halves: float32 [16384, 1024], P('wide', 'narrow')
The draws below stay inside these ranges and needn't reach their ends.
Inputs may be any that keep to these rules, and one draw needn't show every extreme that they name: Each block of 2048 rows of moments is symmetric.
All inputs are finite; a program needn't handle non-finite values.
Results may differ from the reference program's by a relative error of at most 0.0001.
Values sent between devices are 32-bit elements; how exact they have to be, the bound alone decides.
No kernel may reach another device: no remote copies, remote signals or barrier semaphores. Data moves between devices by JAX's collectives and lax.ppermute only.
A program may use at most 64 MiB of HBM per device.

```python
import jax
import jax.numpy as jnp
from jax import lax

M = 2048
K = 1024
GROUPS = 8


def draw_moments(key, part):
    base_key = jax.random.fold_in(jax.random.fold_in(key, 11), 0)
    entries = jax.random.normal(base_key, (GROUPS, M, M), jnp.float32)
    symmetric = (entries + jnp.swapaxes(entries, 1, 2)) * 0.7071
    return symmetric.reshape(GROUPS * M, M)


def with_ends(values, rng, least, top_value):
    place = [jax.random.randint(jax.random.fold_in(rng, axis), (), 0, length) for axis, length in enumerate(values.shape)]
    longest = values.shape.index(max(values.shape))
    beside = place[:longest] + [(place[longest] + 1) % values.shape[longest]] + place[longest + 1:]
    return values.at[tuple(place)].set(least).at[tuple(beside)].set(top_value)


def block_scale(stream_key, dims, cuts, low, largest):
    gain = 1.0
    for position, blocks in cuts:
        heights = jax.random.uniform(jax.random.fold_in(jax.random.fold_in(stream_key, 6), position), (blocks,), jnp.float32, low / len(cuts), largest / len(cuts))
        gain = gain * jnp.repeat(jnp.exp(heights), dims[position] // blocks).reshape((-1,) + (1,) * (len(dims) - 1 - position))
    return gain


def gaussian(own_key, dims, scale, limit, pieces=(), held_as=jnp.bfloat16):
    values = jax.random.normal(own_key, dims, jnp.float32) * scale
    if len(pieces) > 0:
        values = block_scale(own_key, dims, pieces, -0.22, 0.18) * values
    return jnp.clip(values, min=-limit, max=limit).astype(held_as)


def setup_inputs(seed: int = 0) -> dict:
    key_list = jax.random.split(jax.random.key(seed), 4)
    return {
        "moments": draw_moments(jax.random.fold_in(key_list[3], 71), 0),
        "eigen_basis": gaussian(key_list[1], (GROUPS * M, M), M ** -0.5, 0.125, ((0, 32), (1, 16)), jnp.float32),
        "slot_order": with_ends((jax.random.randint(key_list[2], (GROUPS,), 0, 2) < 1).astype(jnp.int32), jax.random.fold_in(key_list[2], 1), 0, 1),
    }


def reference(moments, eigen_basis, slot_order):
    outputs = []
    for subproblem in range(GROUPS):
        matrix = moments[subproblem * M:(subproblem + 1) * M]
        vectors = eigen_basis[subproblem * M:(subproblem + 1) * M]
        product = jnp.dot(matrix, vectors, precision=lax.Precision.HIGHEST, preferred_element_type=jnp.float32)
        first_block = jnp.dot(vectors[:, :K].T, product[:, :K], precision=lax.Precision.HIGHEST, preferred_element_type=jnp.float32)
        second = jnp.dot(vectors[:, K:].T, product[:, K:], precision=lax.Precision.HIGHEST, preferred_element_type=jnp.float32)
        swapped = slot_order[subproblem] == 1
        outputs.append(jnp.where(swapped, second, first_block))
        outputs.append(jnp.where(swapped, first_block, second))
    return jnp.concatenate(outputs, axis=0)
```

```python
import functools

import jax
import jax.numpy as jnp
from jax import lax
from jax.experimental import pallas as pl
from jax.experimental.pallas import tpu as pltpu
from jax.sharding import Mesh
from jax.sharding import PartitionSpec as P

ROW = ("zl", "xh")
COL = ("y", "xl", "c")


def split(x):
    high = x.astype(jnp.bfloat16)
    return high, (x - high.astype(jnp.float32)).astype(jnp.bfloat16)


def product(left, right, dims):
    left_high, left_low = left
    right_high, right_low = right
    dot = functools.partial(lax.dot_general, dimension_numbers=(dims, ((), ())), preferred_element_type=jnp.float32)
    return dot(left_high, right_high) + (dot(left_high, right_low) + dot(left_low, right_high))


def image_kernel(swap_ref, a_ref, v_ref, z_ref):
    swap = swap_ref[0]
    rows = [split(a_ref[part]) for part in range(4)]
    for slot in range(2):
        for block in range(2):
            cols = split(v_ref[(slot ^ swap) * 2 + block])
            for part in range(4):
                z_ref[slot * 2 + block, part * 128 : (part + 1) * 128, :] = product(rows[part], cols, ((0,), (0,)))


def image(swap, a, v):
    return pl.pallas_call(
        image_kernel,
        out_shape=jax.ShapeDtypeStruct((4, 512, 128), jnp.float32),
        in_specs=[pl.BlockSpec(memory_space=pltpu.SMEM)] + [pl.BlockSpec(memory_space=pltpu.VMEM)] * 2,
        out_specs=pl.BlockSpec(memory_space=pltpu.VMEM),
        cost_estimate=pl.CostEstimate(flops=6 * 512**3, bytes_accessed=3 * 2**20, transcendentals=0),
    )(swap, a, v)


def project_kernel(half_ref, v_ref, *refs):
    z_refs, y_ref = refs[:-1], refs[-1]
    half = half_ref[0]
    pieces = len(z_refs)
    depth = 512 // pieces
    for block in range(2):
        rows = split(v_ref[half * 2 + block])
        for part in range(4):
            total = None
            for piece in range(pieces):
                cut = slice(piece * depth, (piece + 1) * depth)
                term = product((rows[0][:, cut], rows[1][:, cut]), split(z_refs[piece][part]), ((1,), (0,)))
                total = term if total is None else total + term
            y_ref[block * 2, :, part * 128 : (part + 1) * 128] = total[:64]
            y_ref[block * 2 + 1, :, part * 128 : (part + 1) * 128] = total[64:]


def project(half, v, z):
    return pl.pallas_call(
        project_kernel,
        out_shape=jax.ShapeDtypeStruct((4, 64, 512), jnp.float32),
        in_specs=[pl.BlockSpec(memory_space=pltpu.SMEM)] + [pl.BlockSpec(memory_space=pltpu.VMEM)] * (1 + len(z)),
        out_specs=pl.BlockSpec(memory_space=pltpu.VMEM),
        cost_estimate=pl.CostEstimate(flops=3 * 512**3, bytes_accessed=2 * 2**20, transcendentals=0),
    )(half, v, *z)


def exchange(x, axes):
    return lax.all_to_all(x, axes, 0, 0, tiled=True)


def pair(x, axis):
    other = lax.ppermute(x, axis, [(0, 1), (1, 0)])
    first = lax.axis_index(axis) == 0
    return jnp.where(first, jnp.stack([x, other]), jnp.stack([other, x]))


def body(moments, basis, slot_order):
    swap = lax.dynamic_slice_in_dim(slot_order, lax.axis_index("g"), 1)
    half = lax.axis_index("zl").astype(jnp.int32) ^ swap
    basis_y = exchange(jnp.broadcast_to(basis, (4, 512, 128)), "y")
    moments_q = jnp.swapaxes(pair(pair(moments, "xl"), "c"), 0, 1).reshape(4, 512, 128)

    turned = basis.T.reshape(2, 64, 512)
    x_pos = lax.axis_index("xl")
    c_pos = lax.axis_index("c")
    got = []
    for step in range(2):
        routes = [(x * 2 + c, c * 2 + (x ^ step)) for x in range(2) for c in range(2)]
        got.append(lax.ppermute(lax.dynamic_index_in_dim(turned, x_pos ^ step, 0, keepdims=False), ("xl", "c"), routes))
    mixed = jnp.where(c_pos == 0, jnp.concatenate(got, 0), jnp.concatenate(got[::-1], 0))
    basis_rows = exchange(exchange(jnp.broadcast_to(mixed, (4, 128, 512)), ROW), "y")

    partial = exchange(image(swap, moments_q, basis_y), ROW)
    total = (partial[0] + partial[1]) + (partial[2] + partial[3])
    z = [lax.all_gather(total[i * 256 : (i + 1) * 256], ("xl", "c"), axis=0) for i in range(2)]
    out = exchange(project(half, basis_rows, z), "y")
    return ((out[0] + out[1]) + (out[2] + out[3])).T


def solution(mesh):
    torus = Mesh(mesh.devices.reshape(mesh.shape["wide"] // 4, 2, 2, 4, 2, 2), ("g", *ROW, *COL))
    spec = P(("g", *ROW), COL)
    return jax.shard_map(body, mesh=torus, in_specs=(spec, spec, P()), out_specs=spec, check_vma=False)
```

```python
import functools

import jax
import jax.numpy as jnp
from jax import lax
from jax.experimental import pallas as pl
from jax.experimental.pallas import tpu as pltpu
from jax.sharding import Mesh
from jax.sharding import PartitionSpec as P


ROW = ("zl", "xh")
COL = ("y", "xl", "c")


def split(x):
    high = x.astype(jnp.bfloat16)
    return high, (x - high.astype(jnp.float32)).astype(jnp.bfloat16)


def product(left, right, dims):
    left_high, left_low = left
    right_high, right_low = right
    dot = functools.partial(lax.dot_general, dimension_numbers=(dims, ((), ())), preferred_element_type=jnp.float32)
    return dot(left_high, right_high) + (dot(left_high, right_low) + dot(left_low, right_high))


SMALL = pltpu.CompilerParams(vmem_limit_bytes=24 * 2**20)
IN_VMEM = pl.BlockSpec(memory_space=pltpu.VMEM)
IN_SMEM = pl.BlockSpec(memory_space=pltpu.SMEM)


def image_kernel(place_ref, *refs):
    a_refs, v_ref, z_ref = refs[:4], refs[4], refs[5]
    swap, column = place_ref[0], place_ref[1]
    rows = [split(a_ref[...]) for a_ref in a_refs]
    for slot in range(2):
        for block in range(2):
            cols = split(v_ref[(slot ^ swap) * 2 + block])
            for part in range(4):
                start = pl.multiple_of((column ^ part) * 128, 128)
                z_ref[slot * 2 + block, pl.ds(start, 128), :] = product(rows[part], cols, ((0,), (0,)))


def image(place, a, v):
    return pl.pallas_call(
        image_kernel,
        out_shape=jax.ShapeDtypeStruct((4, 512, 128), jnp.float32),
        in_specs=[IN_SMEM] + [IN_VMEM] * 5,
        out_specs=IN_VMEM,
        compiler_params=SMALL,
        cost_estimate=pl.CostEstimate(flops=6 * 512**3, bytes_accessed=3 * 2**20, transcendentals=0),
    )(place, *a, v)


def project_kernel(half_ref, v_ref, *refs):
    z_refs, y_ref = refs[:-1], refs[-1]
    half = half_ref[0]
    depth = 512 // len(z_refs)
    for block in range(2):
        rows = split(v_ref[half * 2 + block])
        for part in range(4):
            total = None
            for piece, z_ref in enumerate(z_refs):
                cut = slice(piece * depth, (piece + 1) * depth)
                term = product((rows[0][:, cut], rows[1][:, cut]), split(z_ref[part]), ((1,), (0,)))
                total = term if total is None else total + term
            y_ref[block * 2, :, part * 128 : (part + 1) * 128] = total[:64]
            y_ref[block * 2 + 1, :, part * 128 : (part + 1) * 128] = total[64:]


def project(half, v, z):
    return pl.pallas_call(
        project_kernel,
        out_shape=jax.ShapeDtypeStruct((4, 64, 512), jnp.float32),
        in_specs=[IN_SMEM] + [IN_VMEM] * (1 + len(z)),
        out_specs=IN_VMEM,
        compiler_params=SMALL,
        cost_estimate=pl.CostEstimate(flops=3 * 512**3, bytes_accessed=2 * 2**20, transcendentals=0),
    )(half, v, *z)


def order_kernel(place_ref, *refs):
    for part, x_ref in enumerate(refs[:4]):
        refs[4][place_ref[0] ^ part] = x_ref[...]


def in_order(place, parts):
    return pl.pallas_call(
        order_kernel,
        out_shape=jax.ShapeDtypeStruct((4, *parts[0].shape), jnp.float32),
        in_specs=[IN_SMEM] + [IN_VMEM] * 4,
        out_specs=IN_VMEM,
        compiler_params=SMALL,
        cost_estimate=pl.CostEstimate(flops=2**20, bytes_accessed=2 * 2**20, transcendentals=0),
    )(place, *parts)


def exchange(x, axes):
    return lax.all_to_all(x, axes, 0, 0, tiled=True)


FLIP = [(0, 1), (1, 0)]


def body(moments, basis, slot_order):
    swap = lax.dynamic_slice_in_dim(slot_order, lax.axis_index("g"), 1)
    half = lax.axis_index("zl").astype(jnp.int32) ^ swap
    x_pos = lax.axis_index("xl")
    c_pos = lax.axis_index("c")
    row = lax.axis_index(ROW).astype(jnp.int32).reshape(1)
    basis_y = exchange(jnp.broadcast_to(basis, (4, 512, 128)), "y")
    by_x = lax.ppermute(moments, "xl", FLIP)
    by_c = lax.ppermute(moments, "c", FLIP)
    by_xc = lax.ppermute(by_x, "c", FLIP)

    turned = basis.T.reshape(2, 64, 512)
    got = []
    for step in range(2):
        routes = [(x * 2 + c, c * 2 + (x ^ step)) for x in range(2) for c in range(2)]
        piece = lax.dynamic_index_in_dim(turned, x_pos ^ step, 0, keepdims=False)
        got.append(lax.ppermute(piece, ("xl", "c"), routes))
    mixed = jnp.where(c_pos == 0, jnp.concatenate(got, 0), jnp.concatenate(got[::-1], 0))

    place = jnp.concatenate([swap, (x_pos * 2 + c_pos).astype(jnp.int32).reshape(1)])
    partial = image(place, (moments, by_c, by_x, by_xc), basis_y)
    summed = exchange(partial, ROW)

    parts = [mixed] + [lax.ppermute(mixed, ROW, [(p, p ^ m) for p in range(4)]) for m in (1, 2, 3)]
    basis_rows = exchange(in_order(row, parts), "y")

    total = (summed[0] + summed[1]) + (summed[2] + summed[3])
    z = [lax.all_gather(total[i * 256 : (i + 1) * 256], ("xl", "c"), axis=0) for i in range(2)]
    out = exchange(project(half, basis_rows, z), "y")
    return ((out[0] + out[1]) + (out[2] + out[3])).T


def solution(mesh):
    torus = Mesh(mesh.devices.reshape(mesh.shape["wide"] // 4, 2, 2, 4, 2, 2), ("g", *ROW, *COL))
    spec = P(("g", *ROW), COL)
    return jax.shard_map(body, mesh=torus, in_specs=(spec, spec, P()), out_specs=spec, check_vma=False)
```

```python
import functools

import jax
import jax.numpy as jnp
from jax import lax
from jax.experimental import pallas as pl
from jax.experimental.pallas import tpu as pltpu
from jax.sharding import Mesh
from jax.sharding import PartitionSpec as P


ROW = ("zl", "xh")
COL = ("y", "xl", "c")


def split(x):
    high = x.astype(jnp.bfloat16)
    return high, (x - high.astype(jnp.float32)).astype(jnp.bfloat16)


def product(left, right, dims):
    left_high, left_low = left
    right_high, right_low = right
    dot = functools.partial(lax.dot_general, dimension_numbers=(dims, ((), ())), preferred_element_type=jnp.float32)
    return dot(left_high, right_high) + (dot(left_high, right_low) + dot(left_low, right_high))


SMALL = pltpu.CompilerParams(vmem_limit_bytes=24 * 2**20)
IN_VMEM = pl.BlockSpec(memory_space=pltpu.VMEM)
IN_SMEM = pl.BlockSpec(memory_space=pltpu.SMEM)


def at(axis):
    return lax.axis_index(axis).astype(jnp.int32)


def image_kernel(swap, *refs):
    a_refs, v_ref, z_ref = refs[:4], refs[4], refs[5]
    column = at("xl") * 2 + at("c")
    rows = split(jnp.concatenate([a_ref[...] for a_ref in a_refs], axis=1))
    for slot in range(2):
        cols = split(jnp.concatenate([v_ref[(slot ^ swap) * 2], v_ref[(slot ^ swap) * 2 + 1]], axis=1))
        result = product(rows, cols, ((0,), (0,)))
        for part in range(4):
            start = pl.multiple_of((column ^ part) * 128, 128)
            for block in range(2):
                z_ref[slot * 2 + block, pl.ds(start, 128), :] = result[
                    part * 128 : (part + 1) * 128, block * 128 : (block + 1) * 128
                ]


def image(swap, a, v):
    return pl.pallas_call(
        functools.partial(image_kernel, swap),
        out_shape=jax.ShapeDtypeStruct((4, 512, 128), jnp.float32),
        in_specs=[IN_VMEM] * 5,
        out_specs=IN_VMEM,
        compiler_params=SMALL,
        cost_estimate=pl.CostEstimate(flops=6 * 512**3, bytes_accessed=3 * 2**20, transcendentals=0),
    )(*a, v)


def project_kernel(*refs):
    kept_refs, other_ref, mixed_ref, z_refs, y_ref = refs[:2], refs[2], refs[3], refs[4:8], refs[8]
    c_pos = at("c")
    column, block_pos = at("xl") * 2 + c_pos, at("y") % 2
    cols = split(jnp.concatenate([z_ref[...] for z_ref in z_refs], axis=1))
    own = pl.ds(pl.multiple_of(c_pos * 64, 64), 64)
    kept = jnp.where((at("xh") ^ block_pos) == 0, kept_refs[0][own, :], kept_refs[1][own, :])
    rows = split(jnp.concatenate([kept, mixed_ref[0], other_ref[own, :], mixed_ref[1]], axis=0))
    result = product(rows, cols, ((1,), (0,)))
    for block in range(2):
        for side in range(2):
            piece = (block_pos ^ block) * 2 + (c_pos ^ side)
            for part in range(4):
                start = pl.multiple_of((column ^ part) * 128, 128)
                first = (block * 2 + side) * 64
                y_ref[piece, :, pl.ds(start, 128)] = result[first : first + 64, part * 128 : (part + 1) * 128]


def project(kept, other, mixed, z):
    return pl.pallas_call(
        project_kernel,
        out_shape=jax.ShapeDtypeStruct((4, 64, 512), jnp.float32),
        in_specs=[IN_VMEM] * 8,
        out_specs=IN_VMEM,
        compiler_params=SMALL,
        cost_estimate=pl.CostEstimate(flops=3 * 512**3, bytes_accessed=2 * 2**20, transcendentals=0),
    )(*kept, other, mixed, *z)


def exchange(x, axes):
    return lax.all_to_all(x, axes, 0, 0, tiled=True)


def index(*bits):
    return functools.reduce(lambda total, bit: total * 2 + bit, bits, 0)


def turning(swap, step):
    routes = []
    for source in range(64):
        zl, xh, high, low, xl, c = (source >> shift & 1 for shift in range(5, -1, -1))
        routes.append((source, index(high ^ swap, xh ^ step, zl, low, c, xl)))
    return routes


FLIP = [(0, 1), (1, 0)]


def branch(swap, moments, basis):
    basis_y = exchange(jnp.broadcast_to(basis, (4, 512, 128)), "y")
    turned = basis.T
    by_x = lax.ppermute(moments, "xl", FLIP)
    by_c = lax.ppermute(moments, "c", FLIP)
    by_xc = lax.ppermute(by_x, "c", FLIP)
    kept = [lax.ppermute(turned, (*ROW, *COL), turning(swap, m)) for m in range(2)]
    partial = image(swap, (moments, by_c, by_x, by_xc), basis_y)
    summed = exchange(partial, ROW)

    low = at("y") % 2
    keep_first = (at("xh") ^ low) == 0
    away = jnp.where(keep_first, kept[1], kept[0])
    other = lax.ppermute(away, "y", [(y, y ^ 1) for y in range(4)])
    c_pos = lax.axis_index("c")
    cross = jnp.stack([jnp.where(keep_first, kept[0], kept[1]), other]).reshape(2, 2, 64, 512)
    mixed = lax.ppermute(lax.dynamic_index_in_dim(cross, 1 - c_pos, 1, keepdims=False), "c", FLIP)

    total = (summed[0] + summed[1]) + (summed[2] + summed[3])
    z_x = lax.ppermute(total, "xl", FLIP)
    z_c = lax.ppermute(total, "c", FLIP)
    z_xc = lax.ppermute(z_x, "c", FLIP)
    out = exchange(project(kept, other, mixed, (total, z_c, z_x, z_xc)), "y")
    return ((out[0] + out[1]) + (out[2] + out[3])).T


def body(moments, basis, slot_order):
    swap = lax.dynamic_index_in_dim(slot_order, lax.axis_index("g"), 0, keepdims=False)
    return lax.cond(swap == 0, functools.partial(branch, 0), functools.partial(branch, 1), moments, basis)


def solution(mesh):
    torus = Mesh(mesh.devices.reshape(mesh.shape["wide"] // 4, 2, 2, 4, 2, 2), ("g", *ROW, *COL))
    spec = P(("g", *ROW), COL)
    return jax.shard_map(body, mesh=torus, in_specs=(spec, spec, P()), out_specs=spec, check_vma=False)
```

```python
import functools

import jax
import jax.numpy as jnp
from jax import lax
from jax.experimental import pallas as pl
from jax.experimental.pallas import tpu as pltpu
from jax.sharding import Mesh
from jax.sharding import PartitionSpec as P


ROW = ("zl", "xh")
COL = ("y", "xl", "c")


def split(x):
    high = x.astype(jnp.bfloat16)
    return high, (x - high.astype(jnp.float32)).astype(jnp.bfloat16)


def product(left, right, dims):
    left_high, left_low = left
    right_high, right_low = right
    dot = functools.partial(lax.dot_general, dimension_numbers=(dims, ((), ())), preferred_element_type=jnp.float32)
    return dot(left_high, right_high) + (dot(left_high, right_low) + dot(left_low, right_high))


SMALL = pltpu.CompilerParams(vmem_limit_bytes=24 * 2**20)
IN_VMEM = pl.BlockSpec(memory_space=pltpu.VMEM)
IN_SMEM = pl.BlockSpec(memory_space=pltpu.SMEM)


def at(axis):
    return lax.axis_index(axis).astype(jnp.int32)


def image_kernel(swap, *refs):
    a_refs, v_ref, z_ref = refs[:4], refs[4], refs[5]
    column = at("xl") * 2 + at("c")
    rows = split(jnp.concatenate([a_ref[...] for a_ref in a_refs], axis=1))
    for slot in range(2):
        cols = split(jnp.concatenate([v_ref[(slot ^ swap) * 2], v_ref[(slot ^ swap) * 2 + 1]], axis=1))
        result = product(rows, cols, ((0,), (0,)))
        for part in range(4):
            start = pl.multiple_of((column ^ part) * 128, 128)
            for block in range(2):
                z_ref[slot * 2 + block, pl.ds(start, 128), :] = result[
                    part * 128 : (part + 1) * 128, block * 128 : (block + 1) * 128
                ]


def image(swap, a, v):
    return pl.pallas_call(
        functools.partial(image_kernel, swap),
        out_shape=jax.ShapeDtypeStruct((4, 512, 128), jnp.float32),
        in_specs=[IN_VMEM] * 5,
        out_specs=IN_VMEM,
        compiler_params=SMALL,
        cost_estimate=pl.CostEstimate(flops=6 * 512**3, bytes_accessed=3 * 2**20, transcendentals=0),
    )(*a, v)


def project_kernel(swap, *refs):
    kept_refs, other_ref, mixed_ref, z_refs, y_ref = refs[:2], refs[2], refs[3], refs[4:8], refs[8]
    c_pos = at("c")
    column, block_pos = at("xl") * 2 + c_pos, at("y") % 2
    first_block = block_pos ^ (at("y") // 2) ^ at("zl") ^ swap
    cols = split(jnp.concatenate([z_ref[...] for z_ref in z_refs], axis=1))
    own = pl.ds(pl.multiple_of(c_pos * 64, 64), 64)
    kept = jnp.where((at("xh") ^ block_pos) == 0, kept_refs[0][own, :], kept_refs[1][own, :])
    rows = split(jnp.concatenate([kept, mixed_ref[0], other_ref[own, :], mixed_ref[1]], axis=0))
    result = product(rows, cols, ((1,), (0,)))
    for block in range(2):
        for side in range(2):
            piece = (first_block ^ block) * 2 + (c_pos ^ side)
            for part in range(4):
                start = pl.multiple_of((column ^ part) * 128, 128)
                first = (block * 2 + side) * 64
                y_ref[piece, :, pl.ds(start, 128)] = result[first : first + 64, part * 128 : (part + 1) * 128]


def project(swap, kept, other, mixed, z):
    return pl.pallas_call(
        functools.partial(project_kernel, swap),
        out_shape=jax.ShapeDtypeStruct((4, 64, 512), jnp.float32),
        in_specs=[IN_VMEM] * 8,
        out_specs=IN_VMEM,
        compiler_params=SMALL,
        cost_estimate=pl.CostEstimate(flops=3 * 512**3, bytes_accessed=2 * 2**20, transcendentals=0),
    )(*kept, other, mixed, *z)


def exchange(x, axes):
    return lax.all_to_all(x, axes, 0, 0, tiled=True)


def index(*bits):
    return functools.reduce(lambda total, bit: total * 2 + bit, bits, 0)


def turning(swap, step):
    routes = []
    for source in range(64):
        zl, xh, high, low, xl, c = (source >> shift & 1 for shift in range(5, -1, -1))
        routes.append((source, index(high ^ swap, xh ^ step, zl, low ^ zl ^ high, c, xl)))
    return routes


FLIP = [(0, 1), (1, 0)]


def branch(swap, moments, basis):
    basis_y = exchange(jnp.broadcast_to(basis, (4, 512, 128)), "y")
    turned = basis.T
    by_x = lax.ppermute(moments, "xl", FLIP)
    by_c = lax.ppermute(moments, "c", FLIP)
    by_xc = lax.ppermute(by_x, "c", FLIP)
    kept = [lax.ppermute(turned, (*ROW, *COL), turning(swap, m)) for m in range(2)]
    partial = image(swap, (moments, by_c, by_x, by_xc), basis_y)
    summed = exchange(partial, ROW)

    low = at("y") % 2
    keep_first = (at("xh") ^ low) == 0
    away = jnp.where(keep_first, kept[1], kept[0])
    other = lax.ppermute(away, "y", [(y, y ^ 1) for y in range(4)])
    c_pos = lax.axis_index("c")
    cross = jnp.stack([jnp.where(keep_first, kept[0], kept[1]), other]).reshape(2, 2, 64, 512)
    mixed = lax.ppermute(lax.dynamic_index_in_dim(cross, 1 - c_pos, 1, keepdims=False), "c", FLIP)

    total = (summed[0] + summed[1]) + (summed[2] + summed[3])
    z_x = lax.ppermute(total, "xl", FLIP)
    z_c = lax.ppermute(total, "c", FLIP)
    z_xc = lax.ppermute(z_x, "c", FLIP)
    out = exchange(project(swap, kept, other, mixed, (total, z_c, z_x, z_xc)), "y")
    return ((out[0] + out[1]) + (out[2] + out[3])).T


def body(moments, basis, slot_order):
    swap = lax.dynamic_index_in_dim(slot_order, lax.axis_index("g"), 0, keepdims=False)
    return lax.cond(swap == 0, functools.partial(branch, 0), functools.partial(branch, 1), moments, basis)


def solution(mesh):
    torus = Mesh(mesh.devices.reshape(mesh.shape["wide"] // 4, 2, 2, 4, 2, 2), ("g", *ROW, *COL))
    spec = P(("g", *ROW), COL)
    return jax.shard_map(body, mesh=torus, in_specs=(spec, spec, P()), out_specs=spec, check_vma=False)
```

```python
import functools

import jax
import jax.numpy as jnp
from jax import lax
from jax.experimental import pallas as pl
from jax.experimental.pallas import tpu as pltpu
from jax.sharding import Mesh
from jax.sharding import PartitionSpec as P


ROW = ("zl", "xh")
COL = ("y", "xl", "c")


def split(x):
    high = x.astype(jnp.bfloat16)
    return high, (x - high.astype(jnp.float32)).astype(jnp.bfloat16)


def product(left, right, dims):
    left_high, left_low = left
    right_high, right_low = right
    dot = functools.partial(lax.dot_general, dimension_numbers=(dims, ((), ())), preferred_element_type=jnp.float32)
    return dot(left_high, right_high) + (dot(left_high, right_low) + dot(left_low, right_high))


SMALL = pltpu.CompilerParams(vmem_limit_bytes=24 * 2**20)
IN_VMEM = pl.BlockSpec(memory_space=pltpu.VMEM)
IN_SMEM = pl.BlockSpec(memory_space=pltpu.SMEM)


def at(axis):
    return lax.axis_index(axis).astype(jnp.int32)


def image_kernel(swap, *refs):
    a_refs, v_ref, z_ref = refs[:4], refs[4], refs[5]
    column = at("xl") * 2 + at("c")
    rows = split(jnp.concatenate([a_ref[...] for a_ref in a_refs], axis=1))
    for slot in range(2):
        cols = split(jnp.concatenate([v_ref[(slot ^ swap) * 2], v_ref[(slot ^ swap) * 2 + 1]], axis=1))
        result = product(rows, cols, ((0,), (0,)))
        for part in range(4):
            start = pl.multiple_of((column ^ part) * 128, 128)
            for block in range(2):
                z_ref[slot * 2 + block, pl.ds(start, 128), :] = result[
                    part * 128 : (part + 1) * 128, block * 128 : (block + 1) * 128
                ]


def image(swap, a, v):
    return pl.pallas_call(
        functools.partial(image_kernel, swap),
        out_shape=jax.ShapeDtypeStruct((4, 512, 128), jnp.float32),
        in_specs=[IN_VMEM] * 5,
        out_specs=IN_VMEM,
        compiler_params=SMALL,
        cost_estimate=pl.CostEstimate(flops=6 * 512**3, bytes_accessed=3 * 2**20, transcendentals=0),
    )(*a, v)


def project_kernel(swap, *refs):
    kept_refs, other_ref, mixed_ref, z_refs, y_ref = refs[:2], refs[2], refs[3], refs[4:8], refs[8]
    c_pos = at("c")
    column, block_pos = at("xl") * 2 + c_pos, at("y") % 2
    first_block = block_pos ^ (at("y") // 2) ^ at("zl") ^ swap
    cols = split(jnp.concatenate([z_ref[...] for z_ref in z_refs], axis=1))
    own = pl.ds(pl.multiple_of(c_pos * 64, 64), 64)
    kept = jnp.where((at("xh") ^ block_pos) == 0, kept_refs[0][own, :], kept_refs[1][own, :])
    rows = split(jnp.concatenate([kept, mixed_ref[0], other_ref[own, :], mixed_ref[1]], axis=0))
    result = product(rows, cols, ((1,), (0,)))
    for block in range(2):
        for side in range(2):
            piece = (first_block ^ block) * 2 + (c_pos ^ side)
            for part in range(4):
                start = pl.multiple_of((column ^ part) * 128, 128)
                first = (block * 2 + side) * 64
                y_ref[piece, :, pl.ds(start, 128)] = result[first : first + 64, part * 128 : (part + 1) * 128]


def project(swap, kept, other, mixed, z):
    return pl.pallas_call(
        functools.partial(project_kernel, swap),
        out_shape=jax.ShapeDtypeStruct((4, 64, 512), jnp.float32),
        in_specs=[IN_VMEM] * 8,
        out_specs=IN_VMEM,
        compiler_params=SMALL,
        cost_estimate=pl.CostEstimate(flops=3 * 512**3, bytes_accessed=2 * 2**20, transcendentals=0),
    )(*kept, other, mixed, *z)


def exchange(x, axes):
    return lax.all_to_all(x, axes, 0, 0, tiled=True)


def index(*bits):
    return functools.reduce(lambda total, bit: total * 2 + bit, bits, 0)


def turning(swap, step):
    routes = []
    for source in range(64):
        zl, xh, high, low, xl, c = (source >> shift & 1 for shift in range(5, -1, -1))
        routes.append((source, index(high ^ swap, xh ^ step, zl, low ^ zl ^ high, c, xl)))
    return routes


FLIP = [(0, 1), (1, 0)]


def spread_kernel(slot_ref, v_ref, spread_ref, turned_ref, swap_ref):
    swap_ref[0] = slot_ref[at("g")]
    value = v_ref[...]
    for place in range(4):
        spread_ref[place] = value
    turned_ref[...] = value.T


def spread_out(slot_order, v):
    return pl.pallas_call(
        spread_kernel,
        out_shape=(
            jax.ShapeDtypeStruct((4, 512, 128), jnp.float32),
            jax.ShapeDtypeStruct((128, 512), jnp.float32),
            jax.ShapeDtypeStruct((1,), jnp.int32),
        ),
        in_specs=[IN_SMEM, IN_VMEM],
        out_specs=(IN_VMEM, IN_VMEM, IN_SMEM),
        compiler_params=SMALL,
        cost_estimate=pl.CostEstimate(flops=2**20, bytes_accessed=2**21, transcendentals=0),
    )(slot_order, v)


def branch(swap, moments, spread, turned):
    basis_y = exchange(spread, "y")
    by_x = lax.ppermute(moments, "xl", FLIP)
    by_c = lax.ppermute(moments, "c", FLIP)
    by_xc = lax.ppermute(by_x, "c", FLIP)
    kept = [lax.ppermute(turned, (*ROW, *COL), turning(swap, m)) for m in range(2)]
    partial = image(swap, (moments, by_c, by_x, by_xc), basis_y)
    summed = exchange(partial, ROW)

    low = at("y") % 2
    keep_first = (at("xh") ^ low) == 0
    away = jnp.where(keep_first, kept[1], kept[0])
    other = lax.ppermute(away, "y", [(y, y ^ 1) for y in range(4)])
    c_pos = lax.axis_index("c")
    cross = jnp.stack([jnp.where(keep_first, kept[0], kept[1]), other]).reshape(2, 2, 64, 512)
    mixed = lax.ppermute(lax.dynamic_index_in_dim(cross, 1 - c_pos, 1, keepdims=False), "c", FLIP)

    total = (summed[0] + summed[1]) + (summed[2] + summed[3])
    z_x = lax.ppermute(total, "xl", FLIP)
    z_c = lax.ppermute(total, "c", FLIP)
    z_xc = lax.ppermute(z_x, "c", FLIP)
    return exchange(project(swap, kept, other, mixed, (total, z_c, z_x, z_xc)), "y")


def body(moments, basis, slot_order):
    spread, turned, swap = spread_out(slot_order, basis)
    out = lax.switch(swap[0], (functools.partial(branch, 0), functools.partial(branch, 1)), moments, spread, turned)
    return ((out[0] + out[1]) + (out[2] + out[3])).T


def solution(mesh):
    torus = Mesh(mesh.devices.reshape(mesh.shape["wide"] // 4, 2, 2, 4, 2, 2), ("g", *ROW, *COL))
    spec = P(("g", *ROW), COL)
    return jax.shard_map(body, mesh=torus, in_specs=(spec, spec, P()), out_specs=spec, check_vma=False)
```
